32 devices in a mesh: gx: 4 (over x, core), gy: 2 (over y), gz: 4 (over z).
Axes of the slice: x: 2, y: 2, z: 4, core: 2. Of those that a mesh axis runs over, the one named last changes fastest.
Arguments:
- start_field: float32 [256, 128, 1024], P('gx', 'gy', 'gz'), may hold values from -6 to 6
- right_side: float32 [256, 128, 1024], P('gx', 'gy', 'gz'), may hold values from -6 to 6
Outputs:
- corrected: float32 [256, 128, 1024], P('gx', 'gy', 'gz')
The draws below stay inside these ranges and needn't reach their ends.
All inputs are finite; a program needn't handle non-finite values.
Results may differ from the reference program's by a relative error of at most 0.00002.
Values sent between devices are 32-bit elements; how exact they have to be, the bound alone decides.
A program may use at most 128 MiB of HBM per device.

```python
import jax
import jax.numpy as jnp
from jax import lax

FINE_SWEEPS = 2
COARSE_SWEEPS = 4
NX = 256
NY = 128
NZ = 1024


def draw_right_side(key, part):
    noise_field = jnp.clip(jax.random.normal(key, (NX, NY, NZ), jnp.float32), -6.0, 6.0)
    return noise_field


def levels(stream_key, dims, shards, smallest, top_value):
    def one(position, shards_of):
        draws = jax.random.uniform(jax.random.fold_in(jax.random.fold_in(stream_key, 6), position), (shards_of,), jnp.float32, smallest / len(shards), top_value / len(shards))
        return jnp.repeat(jnp.exp(draws), dims[position] // shards_of).reshape((-1,) + (1,) * (len(dims) - position - 1))

    factor_of = one(*shards[0])
    for cut in shards[1:]:
        factor_of = factor_of * one(*cut)
    return factor_of


def bell_draw(key, shape, spread, reach, pieces=(), kind=jnp.bfloat16):
    drawn = jax.random.normal(key, shape, jnp.float32) * spread
    if len(pieces) > 0:
        drawn = levels(key, shape, pieces, -0.22, 0.18) * drawn
    return jnp.clip(drawn, min=-reach, max=reach).astype(kind)


def setup_inputs(seed: int = 0) -> dict:
    seeds = jax.random.split(jax.random.key(seed), 3)
    start_field = bell_draw(seeds[0], (NX, NY, NZ), 1.0, 6.0, ((0, 4), (1, 2), (2, 4)), jnp.float32)
    right_side = draw_right_side(jax.random.fold_in(seeds[2], 71), 0)
    return {"start_field": start_field, "right_side": right_side}


relaxation = 6.0 / 7.0


def apply_stencil(values):
    padded = jnp.pad(values, 1)
    beside = padded[2:, 1:-1, 1:-1] + padded[:-2, 1:-1, 1:-1]
    beside = beside + padded[1:-1, 2:, 1:-1] + padded[1:-1, :-2, 1:-1]
    beside = beside + padded[1:-1, 1:-1, 2:] + padded[1:-1, 1:-1, :-2]
    return 6.0 * values - beside


def restrict_axis(values, which_axis):
    length = values.shape[which_axis]
    half_len = length // 2
    even_rows = lax.slice_in_dim(values, 0, length, 2, which_axis)
    odd_rows = lax.slice_in_dim(values, 1, length, 2, which_axis)
    zero_row = jnp.zeros_like(lax.slice_in_dim(even_rows, 0, 1, 1, which_axis))
    following = jnp.concatenate([lax.slice_in_dim(even_rows, 1, half_len, 1, which_axis), zero_row], which_axis)
    return 0.25 * even_rows + 0.5 * odd_rows + 0.25 * following


def prolong_axis(values, which_axis):
    length = values.shape[which_axis]
    zero_row = jnp.zeros_like(lax.slice_in_dim(values, 0, 1, 1, which_axis))
    previous = jnp.concatenate([zero_row, lax.slice_in_dim(values, 0, length - 1, 1, which_axis)], which_axis)
    even_rows = 0.5 * (previous + values)
    paired = jnp.stack([even_rows, values], which_axis + 1)
    new_shape = list(values.shape)
    new_shape[which_axis] = 2 * length
    return jnp.reshape(paired, new_shape)


def reference(start_field, right_side):
    smoothed = start_field
    for sweep_num in range(FINE_SWEEPS):
        smoothed = smoothed + (relaxation / 6.0) * (right_side - apply_stencil(smoothed))
    residual = right_side - apply_stencil(smoothed)
    coarse_rhs = restrict_axis(restrict_axis(restrict_axis(residual, 0), 1), 2)
    correction = jnp.zeros_like(coarse_rhs)
    for sweep_num in range(COARSE_SWEEPS):
        correction = correction + (relaxation / 1.5) * (coarse_rhs - 0.25 * apply_stencil(correction))
    fine_corr = prolong_axis(prolong_axis(prolong_axis(correction, 0), 1), 2)
    return smoothed + fine_corr
```

```python
import functools

import jax
import jax.numpy as jnp
from jax import lax
from jax.experimental import pallas as pl
from jax.experimental.pallas import tpu as pltpu
from jax.sharding import PartitionSpec as P

FINE_SWEEPS = 2
COARSE_SWEEPS = 4
OMEGA = 6.0 / 7.0
STEP = OMEGA / 1.5
LANES = 128
PAD = 8
AXES = ("gx", "gy", "gz")
MESH = pl.DeviceIdType.MESH
HIGH = lax.Precision.HIGHEST

FACES = ((1, 0, 0), (-1, 0, 0), (0, 1, 0), (0, -1, 0), (0, 0, 1), (0, 0, -1))
EDGES = ((0, 1, 1), (1, 1, 0), (1, 0, 1), (1, 1, 1))
NEIGHBOURS = FACES + EDGES + tuple(tuple(-c for c in d) for d in EDGES)
N_COPIES = 6 * (FINE_SWEEPS + 1) + 4 + 6 * (COARSE_SWEEPS - 1) + 7


def rotated(values, shift):
    return pltpu.roll(values, shift, 1)


def correct_kernel(
    sizes, start_hbm, right_hbm, smooth_hbm, q_ref,
    u0, u1, u2, f, ys, yr, zs, zr, rs, rr, px, rys, ryr, rdr, rzs, rzr, rhs,
    c0, c1, c2, c3, cys, cyr, czs, czr, xyr, xzr, yzr, xyzr, ze,
    local_sem, send_sem, recv_sem,
):
    nt, nx, ny, _ = f.shape
    mx, my = nx // 2, ny // 2
    me = tuple(lax.axis_index(a) for a in AXES)
    lane = lax.broadcasted_iota(jnp.int32, (ny, LANES), 1)
    lane_c = lax.broadcasted_iota(jnp.int32, (my, LANES), 1)

    def there(d):
        found = None
        for at, step, size in zip(me, d, sizes):
            if step:
                one = at < size - 1 if step > 0 else at > 0
                found = one if found is None else jnp.logical_and(found, one)
        return found

    def minus(d):
        return tuple(-c for c in d)

    def device(d):
        return tuple(at + step for at, step in zip(me, d))

    sent = []

    def send(src, dst, d):
        number = len(sent)

        def copy(to):
            return pltpu.make_async_remote_copy(
                src_ref=src, dst_ref=dst, send_sem=send_sem.at[number],
                recv_sem=recv_sem.at[number], device_id=device(to), device_id_type=MESH)

        @pl.when(there(d))
        def _():
            copy(d).start()

        sent.append((copy, d, dst))
        return number

    def arrive(number):
        copy, d, dst = sent[number]

        @pl.when(there(minus(d)))
        def _():
            copy(minus(d)).wait_recv()

        @pl.when(jnp.logical_not(there(minus(d))))
        def _():
            dst[...] = jnp.zeros(dst.shape, dst.dtype)

    loads = []
    for t in range(nt):
        part = pl.ds(t * LANES, LANES)
        loads.append(pltpu.make_async_copy(
            start_hbm.at[:, :, part], u0.at[t, pl.ds(1, nx), pl.ds(PAD, ny), :], local_sem.at[t]))
    for t in range(nt):
        part = pl.ds(t * LANES, LANES)
        loads.append(pltpu.make_async_copy(right_hbm.at[:, :, part], f.at[t], local_sem.at[nt + t]))
    for load in loads:
        load.start()

    barrier = pltpu.get_barrier_semaphore()
    expected = jnp.int32(0)
    for d in NEIGHBOURS:
        @pl.when(there(d))
        def _():
            pl.semaphore_signal(barrier, inc=1, device_id=device(d), device_id_type=MESH)
        expected = expected + there(d).astype(jnp.int32)
    pl.semaphore_wait(barrier, expected)

    mid = pl.ds(PAD, ny)

    def pack_fine(k, x, planes, packs):
        for t in range(nt):
            ys[k, 0, t, pl.ds(x, 1), :] = planes[t][0:1, :]
            ys[k, 1, t, pl.ds(x, 1), :] = planes[t][ny - 1:ny, :]
        low, high = packs
        low = jnp.where(lane == x, rotated(planes[0], x), low)
        high = jnp.where(lane == x, rotated(planes[nt - 1], x + 1), high)
        return low, high

    def send_x(u):
        return [
            send(u.at[:, nx, mid, :], u.at[:, 0, mid, :], (1, 0, 0)),
            send(u.at[:, 1, mid, :], u.at[:, nx + 1, mid, :], (-1, 0, 0)),
        ]

    def send_yz(k, packs):
        zs[k, 0], zs[k, 1] = packs
        return [
            send(ys.at[k, 1], yr.at[k, 0], (0, 1, 0)),
            send(ys.at[k, 0], yr.at[k, 1], (0, -1, 0)),
            send(zs.at[k, 1], zr.at[k, 0], (0, 0, 1)),
            send(zs.at[k, 0], zr.at[k, 1], (0, 0, -1)),
        ]

    def fill_fine(u, k):
        def rows(x, _):
            for t in range(nt):
                u[t, x + 1, PAD - 1:PAD, :] = yr[k, 0, t, pl.ds(x, 1), :]
                u[t, x + 1, PAD + ny:PAD + ny + 1, :] = yr[k, 1, t, pl.ds(x, 1), :]
            return 0
        lax.fori_loop(0, nx, rows, 0, unroll=4)

    def around(u, k, x):
        centers, sums = [], []
        low = rotated(zr[k, 0], lax.rem(LANES - x, LANES))
        high = rotated(zr[k, 1], LANES - 1 - x)
        planes = [u[t, x + 1, mid, :] for t in range(nt)]
        left = [rotated(p, 1) for p in planes]
        right = [rotated(p, LANES - 1) for p in planes]
        for t in range(nt):
            before = jnp.where(lane == 0, left[t - 1] if t else low, left[t])
            after = jnp.where(lane == LANES - 1, right[t + 1] if t < nt - 1 else high, right[t])
            total = u[t, x, mid, :] + u[t, x + 2, mid, :]
            total = total + u[t, x + 1, PAD - 1:PAD - 1 + ny, :] + u[t, x + 1, PAD + 1:PAD + 1 + ny, :]
            sums.append(total + before + after)
        return planes, sums

    zero_pack = (jnp.zeros((ny, LANES), jnp.float32),) * 2

    for load in loads[:nt]:
        load.wait()
    waits = send_x(u0)
    packs = lax.fori_loop(
        0, nx, lambda x, c: pack_fine(0, x, [u0[t, x + 1, mid, :] for t in range(nt)], c), zero_pack)
    waits += send_yz(0, packs)
    for load in loads[nt:]:
        load.wait()

    fields = (u0, u1, u2)
    for k in range(FINE_SWEEPS):
        old, new = fields[k], fields[k + 1]
        for number in waits:
            arrive(number)
        fill_fine(old, k)

        def sweep(x, packs):
            planes, sums = around(old, k, x)
            results = []
            for t in range(nt):
                value = (planes[t] + f[t, x] + sums[t]) * (1.0 - OMEGA)
                new[t, x + 1, mid, :] = value
                results.append(value)
            return pack_fine(k + 1, x, results, packs)

        packs = lax.fori_loop(0, nx, sweep, zero_pack)
        waits = send_x(new) + send_yz(k + 1, packs)

    smooth = fields[FINE_SWEEPS]
    outs = [
        pltpu.make_async_copy(
            smooth.at[t, pl.ds(1, nx), mid, :], smooth_hbm.at[:, :, pl.ds(t * LANES, LANES)],
            local_sem.at[2 * nt + t])
        for t in range(nt)
    ]
    for out in outs:
        out.start()
    for number in waits:
        arrive(number)
    fill_fine(smooth, FINE_SWEEPS)

    def residual(x):
        planes, sums = around(smooth, FINE_SWEEPS, x)
        return tuple(f[t, x] - 6.0 * planes[t] + sums[t] for t in range(nt))

    first = residual(0)
    for t in range(nt):
        rs[t] = first[t]
    rx = send(rs, rr, (-1, 0, 0))

    def restrict_x(at, even, odd, following):
        for t in range(nt):
            value = 0.25 * even[t] + 0.5 * odd[t] + 0.25 * following[t]
            px[t, at, 0:ny, :] = value
            rys[t, pl.ds(at, 1), :] = value[0:1, :]

    def step_x(i, even):
        odd = residual(2 * i + 1)
        following = residual(2 * i + 2)
        restrict_x(i, even, odd, following)
        return following

    even = lax.fori_loop(0, mx - 1, step_x, first)
    odd = residual(nx - 1)
    arrive(rx)
    restrict_x(mx - 1, even, odd, [rr[t] for t in range(nt)])
    ry = send(rys, ryr, (0, -1, 0))
    rd = send(rys, rdr, (0, -1, -1))

    row = lax.broadcasted_iota(jnp.int32, (LANES, LANES), 0)
    col = lax.broadcasted_iota(jnp.int32, (LANES, LANES), 1)

    def weights(fine, coarse, scale):
        gap = fine - 2 * coarse
        outer = jnp.logical_or(gap == 0, gap == 2)
        return jnp.where(gap == 1, 0.5 * scale, jnp.where(outer, 0.25 * scale, 0.0)).astype(jnp.float32)

    down = [weights(row + t * LANES, col, 1.0) for t in range(nt)]
    up = [weights(col + t * LANES, row, 2.0) for t in range(nt)]
    last_row = lax.broadcasted_iota(jnp.int32, (my, LANES), 0) == my - 1

    def step_y(i, pack):
        parts = []
        for t in range(nt):
            evens = px[t, i, pl.ds(0, my, stride=2), :]
            odds = px[t, i, pl.ds(1, my, stride=2), :]
            nexts = jnp.where(last_row, 0.0, pltpu.roll(evens, my - 1, 0))
            parts.append(0.25 * evens + 0.5 * odds + 0.25 * nexts)
        value = jnp.zeros((my, LANES), jnp.float32)
        for t in range(nt):
            value = value + jnp.dot(parts[t], down[t], precision=HIGH, preferred_element_type=jnp.float32)
        rhs[i] = value
        return jnp.where(lane_c == i, rotated(parts[0], i), pack)

    zero_c = jnp.zeros((my, LANES), jnp.float32)
    rzs[...] = lax.fori_loop(0, mx, step_y, zero_c, unroll=2)
    rz = send(rzs, rzr, (0, 0, -1))

    mid_c = pl.ds(PAD, my)

    def pack_coarse(k, i, plane, packs):
        cys[k, 0, pl.ds(i, 1), :] = plane[0:1, :]
        cys[k, 1, pl.ds(i, 1), :] = plane[my - 1:my, :]
        low, high = packs
        low = jnp.where(lane_c == i, rotated(plane, i), low)
        high = jnp.where(lane_c == i, rotated(plane, i + 1), high)
        return low, high

    def send_coarse(c, k, packs):
        czs[k, 0], czs[k, 1] = packs
        return [
            send(c.at[mx, mid_c, :], c.at[0, mid_c, :], (1, 0, 0)),
            send(c.at[1, mid_c, :], c.at[mx + 1, mid_c, :], (-1, 0, 0)),
            send(cys.at[k, 1], cyr.at[k, 0], (0, 1, 0)),
            send(cys.at[k, 0], cyr.at[k, 1], (0, -1, 0)),
            send(czs.at[k, 1], czr.at[k, 0], (0, 0, 1)),
            send(czs.at[k, 0], czr.at[k, 1], (0, 0, -1)),
        ]

    for number in (ry, rd, rz):
        arrive(number)
    lane_x = lax.broadcasted_iota(jnp.int32, (mx, LANES), 1)
    beyond = jnp.where(lane_x == LANES - 1, 0.0625 * rotated(rdr[0], LANES - 1), 0.0)
    for t in range(nt):
        beyond = beyond + 0.25 * jnp.dot(
            ryr[t], down[t], precision=HIGH, preferred_element_type=jnp.float32)
    cys[0, 0] = beyond

    def finish_rhs(i, packs):
        outside = 0.25 * rotated(rzr[...], LANES - 1 - i)
        value = rhs[i] + jnp.where(lane_c == LANES - 1, outside, 0.0)
        value = value + jnp.where(last_row, cys[0, 0, pl.ds(i, 1), :], 0.0)
        value = value * STEP
        rhs[i] = value
        c0[i + 1, mid_c, :] = value
        return pack_coarse(0, i, value, packs)

    packs = lax.fori_loop(0, mx, finish_rhs, (zero_c, zero_c), unroll=2)
    grids = (c0, c1, c2, c3)
    waits = send_coarse(c0, 0, packs)
    for k in range(COARSE_SWEEPS - 1):
        old, new = grids[k], grids[k + 1]
        for number in waits:
            arrive(number)

        def rows(i, _):
            old[i + 1, PAD - 1:PAD, :] = cyr[k, 0, pl.ds(i, 1), :]
            old[i + 1, PAD + my:PAD + my + 1, :] = cyr[k, 1, pl.ds(i, 1), :]
            return 0

        lax.fori_loop(0, mx, rows, 0, unroll=4)

        def sweep_c(i, packs):
            low = rotated(czr[k, 0], lax.rem(LANES - i, LANES))
            high = rotated(czr[k, 1], LANES - 1 - i)
            plane = old[i + 1, mid_c, :]
            total = old[i, mid_c, :] + old[i + 2, mid_c, :]
            total = total + old[i + 1, PAD - 1:PAD - 1 + my, :] + old[i + 1, PAD + 1:PAD + 1 + my, :]
            total = total + jnp.where(lane_c == 0, low, rotated(plane, 1))
            total = total + jnp.where(lane_c == LANES - 1, high, rotated(plane, LANES - 1))
            value = (1.0 - 1.5 * STEP) * plane + rhs[i] + (0.25 * STEP) * total
            new[i + 1, mid_c, :] = value
            return pack_coarse(k + 1, i, value, packs)

        packs = lax.fori_loop(0, mx, sweep_c, (zero_c, zero_c), unroll=2)
        if k < COARSE_SWEEPS - 2:
            waits = send_coarse(new, k + 1, packs)

    k = COARSE_SWEEPS - 1
    last = grids[k]
    czs[k, 1] = packs[1]
    waits = [
        send(last.at[mx, mid_c, :], last.at[0, mid_c, :], (1, 0, 0)),
        send(cys.at[k, 1], cyr.at[k, 0], (0, 1, 0)),
        send(czs.at[k, 1], czr.at[k, 0], (0, 0, 1)),
        send(cys.at[k, 1], xyr, (1, 1, 0)),
        send(czs.at[k, 1], xzr, (1, 0, 1)),
        send(czs.at[k, 1], yzr, (0, 1, 1)),
        send(czs.at[k, 1], xyzr, (1, 1, 1)),
    ]
    for number in waits:
        arrive(number)
    inside = jnp.where(lane_c == 0, rotated(xzr[...], LANES - mx + 1), rotated(czr[k, 0], 1))
    corner = jnp.where(lane_c == 0, rotated(xyzr[...], LANES - mx + 1), rotated(yzr[...], 1))
    ze[mid_c, :] = inside
    ze[0:PAD, :] = corner[my - PAD:my, :]
    last[0, 0:PAD, :] = jnp.broadcast_to(xyr[mx - 1:mx, :], (PAD, LANES))

    def rows_last(i, _):
        last[i + 1, 0:PAD, :] = jnp.broadcast_to(cyr[k, 0, pl.ds(i, 1), :], (PAD, LANES))
        return 0

    lax.fori_loop(0, mx, rows_last, 0, unroll=4)
    lane_e = lax.broadcasted_iota(jnp.int32, (my + PAD, LANES), 1)

    def prolong_z(p, _):
        plane = last[p, 0:PAD + my, :]
        outside = 0.5 * rotated(ze[...], lax.rem(LANES - p, LANES))
        for t in range(nt):
            value = jnp.dot(plane, up[t], precision=HIGH, preferred_element_type=jnp.float32)
            if t == 0:
                value = value + jnp.where(lane_e == 0, outside, 0.0)
            q_ref[p, t] = value
        return 0

    lax.fori_loop(0, mx + 1, prolong_z, 0)

    for copy, d, _ in sent:
        @pl.when(there(d))
        def _():
            copy(d).wait_send()
    for out in outs:
        out.wait()


def add_kernel(per, smooth_ref, q_ref, out_ref, both):
    nt, my = q_ref.shape[1], q_ref.shape[2] - PAD
    base = pl.program_id(0) * per

    def spread(j):
        for t in range(nt):
            here = q_ref[base + j, t, PAD:PAD + my, :]
            before = q_ref[base + j, t, PAD - 1:PAD - 1 + my, :]
            both[j, t, pl.ds(0, my, stride=2), :] = 0.5 * (before + here)
            both[j, t, pl.ds(1, my, stride=2), :] = here

    def run(j, _):
        spread(j)
        return 0

    def add(j, _):
        for t in range(nt):
            part = pl.ds(t * LANES, LANES)
            here = both[j + 1, t]
            out_ref[2 * j, :, part] = smooth_ref[2 * j, :, part] + 0.5 * (both[j, t] + here)
            out_ref[2 * j + 1, :, part] = smooth_ref[2 * j + 1, :, part] + here
        return 0

    lax.fori_loop(0, per + 1, run, 0)
    lax.fori_loop(0, per, add, 0)


def on_device(sizes, start_field, right_side):
    nx, ny, nz = start_field.shape
    nt, mx, my = nz // LANES, nx // 2, ny // 2
    f32 = jnp.float32
    fine = pltpu.VMEM((nt, nx + 2, ny + 2 * PAD, LANES), f32)
    coarse = pltpu.VMEM((mx + 2, my + 2 * PAD, LANES), f32)
    rounds = FINE_SWEEPS + 1
    y_faces = pltpu.VMEM((rounds, 2, nt, nx, LANES), f32)
    z_faces = pltpu.VMEM((rounds, 2, ny, LANES), f32)
    x_plane = pltpu.VMEM((nt, ny, LANES), f32)
    y_rows = pltpu.VMEM((nt, mx, LANES), f32)
    z_pack = pltpu.VMEM((my, LANES), f32)
    smooth, q = pl.pallas_call(
        functools.partial(correct_kernel, sizes),
        out_shape=(
            jax.ShapeDtypeStruct((nx, ny, nz), f32),
            jax.ShapeDtypeStruct((mx + 1, nt, my + PAD, LANES), f32),
        ),
        in_specs=[pl.BlockSpec(memory_space=pl.ANY)] * 2,
        out_specs=(pl.BlockSpec(memory_space=pl.ANY), pl.BlockSpec(memory_space=pltpu.VMEM)),
        scratch_shapes=[
            fine, fine, fine, pltpu.VMEM((nt, nx, ny, LANES), f32),
            y_faces, y_faces, z_faces, z_faces,
            x_plane, x_plane, pltpu.VMEM((nt, mx, ny, LANES), f32),
            y_rows, y_rows, y_rows, z_pack, z_pack, pltpu.VMEM((mx, my, LANES), f32),
            coarse, coarse, coarse, coarse,
            pltpu.VMEM((COARSE_SWEEPS, 2, mx, LANES), f32), pltpu.VMEM((COARSE_SWEEPS, 2, mx, LANES), f32),
            pltpu.VMEM((COARSE_SWEEPS, 2, my, LANES), f32), pltpu.VMEM((COARSE_SWEEPS, 2, my, LANES), f32),
            pltpu.VMEM((mx, LANES), f32), z_pack, z_pack, z_pack, pltpu.VMEM((my + PAD, LANES), f32),
            pltpu.SemaphoreType.DMA((3 * nt,)),
            pltpu.SemaphoreType.DMA((N_COPIES,)),
            pltpu.SemaphoreType.DMA((N_COPIES,)),
        ],
        compiler_params=pltpu.CompilerParams(
            collective_id=0, has_side_effects=True, vmem_limit_bytes=48 * 1024 * 1024),
    )(start_field, right_side)
    per = 8 if mx % 8 == 0 else 1
    block = pl.BlockSpec((2 * per, ny, nz), lambda i: (i, 0, 0))
    return pl.pallas_call(
        functools.partial(add_kernel, per),
        out_shape=jax.ShapeDtypeStruct((nx, ny, nz), f32),
        grid=(mx // per,),
        in_specs=[block, pl.BlockSpec(q.shape, lambda i: (0, 0, 0, 0))],
        out_specs=block,
        scratch_shapes=[pltpu.VMEM((per + 1, nt, ny, LANES), f32)],
    )(smooth, q)


def solution(mesh):
    placed = (P(*AXES), P(*AXES))
    sizes = tuple(mesh.shape[a] for a in AXES)
    return jax.shard_map(
        functools.partial(on_device, sizes), mesh=mesh, in_specs=placed, out_specs=P(*AXES), check_vma=False
    )
```

```python
import functools

import jax
import jax.numpy as jnp
from jax import lax
from jax.experimental import pallas as pl
from jax.experimental.pallas import tpu as pltpu
from jax.sharding import PartitionSpec as P

FINE_SWEEPS = 2
COARSE_SWEEPS = 4
OMEGA = 6.0 / 7.0
STEP = OMEGA / 1.5
LANES = 128
PAD = 8
AXES = ("gx", "gy", "gz")
MESH = pl.DeviceIdType.MESH

FACES = ((1, 0, 0), (-1, 0, 0), (0, 1, 0), (0, -1, 0), (0, 0, 1), (0, 0, -1))
EDGES = ((0, 1, 1), (1, 1, 0), (1, 0, 1), (1, 1, 1))
NEIGHBOURS = FACES + EDGES + tuple(tuple(-c for c in d) for d in EDGES)
N_COPIES = 10 * (FINE_SWEEPS + 1) + 4 + 6 * (COARSE_SWEEPS - 1) + 7


def rotated(values, shift):
    return pltpu.roll(values, shift, 1)


def split_dot(values, matrix):
    high = values.astype(jnp.bfloat16)
    rest = values - high.astype(jnp.float32)
    middle = rest.astype(jnp.bfloat16)
    low = (rest - middle.astype(jnp.float32)).astype(jnp.bfloat16)
    total = jnp.dot(low, matrix, preferred_element_type=jnp.float32)
    total = total + jnp.dot(middle, matrix, preferred_element_type=jnp.float32)
    return total + jnp.dot(high, matrix, preferred_element_type=jnp.float32)


def correct_kernel(
    sizes, start_hbm, right_hbm, u2, q_ref,
    u0, u1, f, ys, yr, zs, zr, zm, rs, rr, px, py, rys, ryr, rdr, rzs, rzr, rhs,
    c0, c1, c2, c3, cys, cyr, czs, czr, czm, xyr, xzr, yzr, xyzr, ze,
    local_sem, send_sem, recv_sem,
):
    nt, nx, ny, _ = f.shape
    mx, my = nx // 2, ny // 2
    half = nx // 2
    me = tuple(lax.axis_index(a) for a in AXES)

    def lanes(rows):
        return lax.broadcasted_iota(jnp.int32, (rows, LANES), 1)

    lane, lane_c = lanes(ny), lanes(my)

    def there(d):
        found = None
        for at, step, size in zip(me, d, sizes):
            if step:
                one = at < size - 1 if step > 0 else at > 0
                found = one if found is None else jnp.logical_and(found, one)
        return found

    def minus(d):
        return tuple(-c for c in d)

    def device(d):
        return tuple(at + step for at, step in zip(me, d))

    sent = []

    def send(src, dst, d):
        number = len(sent)

        def copy(to):
            return pltpu.make_async_remote_copy(
                src_ref=src, dst_ref=dst, send_sem=send_sem.at[number],
                recv_sem=recv_sem.at[number], device_id=device(to), device_id_type=MESH)

        @pl.when(there(d))
        def _():
            copy(d).start()

        sent.append((copy, d, dst))
        return number

    def arrive(number):
        copy, d, dst = sent[number]

        @pl.when(there(minus(d)))
        def _():
            copy(minus(d)).wait_recv()

        @pl.when(jnp.logical_not(there(minus(d))))
        def _():
            dst[...] = jnp.zeros(dst.shape, dst.dtype)

    loads = []
    for into, source in ((u0, start_hbm), (f, right_hbm)):
        for h in range(2):
            for t in range(nt):
                rows = pl.ds(h * half, half)
                to = f.at[t, rows] if into is f else u0.at[t, pl.ds(1 + h * half, half), pl.ds(PAD, ny), :]
                loads.append(pltpu.make_async_copy(
                    source.at[rows, :, pl.ds(t * LANES, LANES)], to, local_sem.at[len(loads)]))
    for load in loads:
        load.start()

    barrier = pltpu.get_barrier_semaphore()
    expected = jnp.int32(0)
    for d in NEIGHBOURS:
        @pl.when(there(d))
        def _():
            pl.semaphore_signal(barrier, inc=1, device_id=device(d), device_id_type=MESH)
        expected = expected + there(d).astype(jnp.int32)
    zs[...] = jnp.zeros(zs.shape, zs.dtype)
    czs[...] = jnp.zeros(czs.shape, czs.dtype)
    pl.semaphore_wait(barrier, expected)

    mid = pl.ds(PAD, ny)

    def pack_lanes(ref, at, place, first, last):
        rows = first.shape[0]
        index = lanes(rows)
        both = rotated(jnp.where(index == LANES - 1, last, first), 2 * place + 1)
        chosen = jnp.logical_or(index == 2 * place, index == 2 * place + 1)
        ref[at] = jnp.where(chosen, both, ref[at])

    def merge_lanes(low, high):
        index = lanes(low.shape[0])
        return jnp.where(lax.rem(index, 2) == 0, low, rotated(high, LANES - 2))

    def pack_fine(k, h, x, planes):
        for t in range(nt):
            ys[k, 0, t, pl.ds(x, 1), :] = planes[t][0:1, :]
            ys[k, 1, t, pl.ds(x, 1), :] = planes[t][ny - 1:ny, :]
        pack_lanes(zs, (k, h), x - h * half, planes[0], planes[nt - 1])

    def send_low(u):
        return send(u.at[:, 1, mid, :], u.at[:, nx + 1, mid, :], (-1, 0, 0))

    def send_high(u):
        return send(u.at[:, nx, mid, :], u.at[:, 0, mid, :], (1, 0, 0))

    def send_yz(k, h):
        rows = pl.ds(h * half, half)
        return [
            send(ys.at[k, 1, :, rows, :], yr.at[k, 0, :, rows, :], (0, 1, 0)),
            send(ys.at[k, 0, :, rows, :], yr.at[k, 1, :, rows, :], (0, -1, 0)),
            send(zs.at[k, h], zr.at[k, h, 0], (0, 0, 1)),
            send(zs.at[k, h], zr.at[k, h, 1], (0, 0, -1)),
        ]

    def fill_fine(u, k, h, waits):
        for number in waits:
            arrive(number)
        zm[k, h] = merge_lanes(zr[k, h, 0], zr[k, h, 1])

        def rows(x, _):
            for t in range(nt):
                u[t, x + 1, PAD - 1:PAD, :] = yr[k, 0, t, pl.ds(x, 1), :]
                u[t, x + 1, PAD + ny:PAD + ny + 1, :] = yr[k, 1, t, pl.ds(x, 1), :]
            return 0
        lax.fori_loop(h * half, (h + 1) * half, rows, 0, unroll=4)

    def around(u, k, h, x):
        sums = []
        outer = rotated(zm[k, h], lax.rem(LANES - 2 * (x - h * half), LANES))
        planes = [u[t, x + 1, mid, :] for t in range(nt)]
        left = [rotated(p, 1) for p in planes]
        right = [rotated(p, LANES - 1) for p in planes]
        for t in range(nt):
            before = jnp.where(lane == 0, left[t - 1] if t else outer, left[t])
            after = jnp.where(lane == LANES - 1, right[t + 1] if t < nt - 1 else outer, right[t])
            total = u[t, x, mid, :] + u[t, x + 2, mid, :]
            total = total + u[t, x + 1, PAD - 1:PAD - 1 + ny, :] + u[t, x + 1, PAD + 1:PAD + 1 + ny, :]
            sums.append(total + before + after)
        return planes, sums

    waits_yz, low_arrival, high_arrival = [None, None], None, None
    for h in range(2):
        for load in loads[h * nt:(h + 1) * nt]:
            load.wait()

        def pack_start(j, _, h=h):
            for x in (2 * j, 2 * j + 1):
                pack_fine(0, h, x, [u0[t, x + 1, mid, :] for t in range(nt)])
            return 0

        lax.fori_loop(h * half // 2, (h + 1) * half // 2, pack_start, 0)
        waits_yz[h] = send_yz(0, h)
        if h == 0:
            high_arrival = send_low(u0)
        else:
            low_arrival = send_high(u0)
    for load in loads[2 * nt:]:
        load.wait()

    fields = (u0, u1, u2)
    for k in range(FINE_SWEEPS):
        old, new = fields[k], fields[k + 1]

        def pair(j, h, old=old, new=new, k=k):
            for x in (2 * j, 2 * j + 1):
                planes, sums = around(old, k, h, x)
                results = []
                for t in range(nt):
                    value = (planes[t] + f[t, x] + sums[t]) * (1.0 - OMEGA)
                    new[t, x + 1, mid, :] = value
                    results.append(value)
                pack_fine(k + 1, h, x, results)

        next_yz = [None, None]
        fill_fine(old, k, 0, waits_yz[0])
        lax.fori_loop(1, half // 2, lambda j, _: (pair(j, 0), 0)[1], 0)
        arrive(low_arrival)
        pair(0, 0)
        next_yz[0] = send_yz(k + 1, 0)
        next_high = send_low(new)
        arrive(high_arrival)
        fill_fine(old, k, 1, waits_yz[1])
        lax.fori_loop(half // 2, nx // 2, lambda j, _: (pair(j, 1), 0)[1], 0)
        next_yz[1] = send_yz(k + 1, 1)
        low_arrival, high_arrival = send_high(new), next_high
        waits_yz = next_yz

    smooth = fields[FINE_SWEEPS]
    k_last = FINE_SWEEPS

    def residual(x, h):
        planes, sums = around(smooth, k_last, h, x)
        return tuple(f[t, x] - 6.0 * planes[t] + sums[t] for t in range(nt))

    def restrict_x(at, even, odd, following):
        for t in range(nt):
            value = 0.25 * even[t] + 0.5 * odd[t] + 0.25 * following[t]
            px[t, at, 0:ny, :] = value
            rys[t, pl.ds(at, 1), :] = value[0:1, :]

    def step_x(i, following, h):
        even, odd = residual(2 * i, h), residual(2 * i + 1, h)
        restrict_x(i, even, odd, following)
        return even

    middle = half // 2
    fill_fine(smooth, k_last, 0, waits_yz[0])
    following = lax.fori_loop(
        0, middle - 2, lambda j, c: step_x(middle - 2 - j, c, 0), residual(half - 2, 0))
    arrive(low_arrival)
    first = step_x(0, following, 0)
    for t in range(nt):
        rs[t] = first[t]
    rx = send(rs, rr, (-1, 0, 0))
    arrive(high_arrival)
    fill_fine(smooth, k_last, 1, waits_yz[1])
    following = lax.fori_loop(
        0, mx - 1 - middle, lambda j, c: step_x(mx - 2 - j, c, 1), residual(nx - 2, 1))
    step_x(middle - 1, following, 0)
    arrive(rx)
    step_x(mx - 1, [rr[t] for t in range(nt)], 1)
    ry = send(rys, ryr, (0, -1, 0))
    rd = send(rys, rdr, (0, -1, -1))

    def weights(fine, coarse, scale):
        gap = fine - 2 * coarse
        outer = jnp.logical_or(gap == 0, gap == 2)
        value = jnp.where(gap == 1, 0.5 * scale, jnp.where(outer, 0.25 * scale, 0.0))
        return value.astype(jnp.bfloat16)

    nz = nt * LANES
    down = weights(
        lax.broadcasted_iota(jnp.int32, (nz, LANES), 0), lax.broadcasted_iota(jnp.int32, (nz, LANES), 1), 1.0)
    up = weights(
        lax.broadcasted_iota(jnp.int32, (LANES, nz), 1), lax.broadcasted_iota(jnp.int32, (LANES, nz), 0), 2.0)
    last_row = lax.broadcasted_iota(jnp.int32, (my, LANES), 0) == my - 1

    def step_y(i, pack):
        for t in range(nt):
            evens = px[t, i, pl.ds(0, my, stride=2), :]
            odds = px[t, i, pl.ds(1, my, stride=2), :]
            nexts = jnp.where(last_row, 0.0, pltpu.roll(evens, my - 1, 0))
            part = 0.25 * evens + 0.5 * odds + 0.25 * nexts
            py[i, :, t * LANES:(t + 1) * LANES] = part
            if t == 0:
                pack = jnp.where(lane_c == i, rotated(part, i), pack)
        return pack

    zero_c = jnp.zeros((my, LANES), jnp.float32)
    rzs[...] = lax.fori_loop(0, mx, step_y, zero_c, unroll=4)
    rz = send(rzs, rzr, (0, 0, -1))
    group = 4 if mx % 4 == 0 else 1

    def step_z(i, _):
        at = pl.ds(i * group, group)
        block = py[at].reshape(group * my, nz)
        rhs[at] = split_dot(block, down).reshape(group, my, LANES)
        return 0

    lax.fori_loop(0, mx // group, step_z, 0)

    mid_c = pl.ds(PAD, my)

    def pack_coarse(k, i, plane):
        cys[k, 0, pl.ds(i, 1), :] = plane[0:1, :]
        cys[k, 1, pl.ds(i, 1), :] = plane[my - 1:my, :]
        pack_lanes(czs, k, i, plane, plane)

    def send_coarse(c, k):
        return [
            send(c.at[mx, mid_c, :], c.at[0, mid_c, :], (1, 0, 0)),
            send(c.at[1, mid_c, :], c.at[mx + 1, mid_c, :], (-1, 0, 0)),
            send(cys.at[k, 1], cyr.at[k, 0], (0, 1, 0)),
            send(cys.at[k, 0], cyr.at[k, 1], (0, -1, 0)),
            send(czs.at[k], czr.at[k, 0], (0, 0, 1)),
            send(czs.at[k], czr.at[k, 1], (0, 0, -1)),
        ]

    for number in (ry, rd, rz):
        arrive(number)
    beyond = jnp.where(lanes(mx) == LANES - 1, 0.0625 * rotated(rdr[0], LANES - 1), 0.0)
    beyond = beyond + 0.25 * split_dot(jnp.concatenate([ryr[t] for t in range(nt)], 1), down)
    cys[0, 0] = beyond

    def finish_rhs(i, _):
        outside = 0.25 * rotated(rzr[...], LANES - 1 - i)
        value = rhs[i] + jnp.where(lane_c == LANES - 1, outside, 0.0)
        value = value + jnp.where(last_row, cys[0, 0, pl.ds(i, 1), :], 0.0)
        value = value * STEP
        rhs[i] = value
        c0[i + 1, mid_c, :] = value
        pack_coarse(0, i, value)
        return 0

    lax.fori_loop(0, mx, finish_rhs, 0, unroll=4)
    grids = (c0, c1, c2, c3)
    waits = send_coarse(c0, 0)
    for k in range(COARSE_SWEEPS - 1):
        old, new = grids[k], grids[k + 1]
        for number in waits:
            arrive(number)
        czm[k] = merge_lanes(czr[k, 0], czr[k, 1])

        def rows(i, _):
            old[i + 1, PAD - 1:PAD, :] = cyr[k, 0, pl.ds(i, 1), :]
            old[i + 1, PAD + my:PAD + my + 1, :] = cyr[k, 1, pl.ds(i, 1), :]
            return 0

        lax.fori_loop(0, mx, rows, 0, unroll=8)

        def sweep_c(i, _):
            outer = rotated(czm[k], lax.rem(LANES - 2 * i, LANES))
            plane = old[i + 1, mid_c, :]
            total = old[i, mid_c, :] + old[i + 2, mid_c, :]
            total = total + old[i + 1, PAD - 1:PAD - 1 + my, :] + old[i + 1, PAD + 1:PAD + 1 + my, :]
            total = total + jnp.where(lane_c == 0, outer, rotated(plane, 1))
            total = total + jnp.where(lane_c == LANES - 1, outer, rotated(plane, LANES - 1))
            value = (1.0 - 1.5 * STEP) * plane + rhs[i] + (0.25 * STEP) * total
            new[i + 1, mid_c, :] = value
            pack_coarse(k + 1, i, value)
            return 0

        lax.fori_loop(0, mx, sweep_c, 0, unroll=4)
        if k < COARSE_SWEEPS - 2:
            waits = send_coarse(new, k + 1)

    k = COARSE_SWEEPS - 1
    last = grids[k]
    waits = [
        send(last.at[mx, mid_c, :], last.at[0, mid_c, :], (1, 0, 0)),
        send(cys.at[k, 1], cyr.at[k, 0], (0, 1, 0)),
        send(czs.at[k], czr.at[k, 0], (0, 0, 1)),
        send(cys.at[k, 1], xyr, (1, 1, 0)),
        send(czs.at[k], xzr, (1, 0, 1)),
        send(czs.at[k], yzr, (0, 1, 1)),
        send(czs.at[k], xyzr, (1, 1, 1)),
    ]
    for number in waits:
        arrive(number)
    turn = LANES - 2 * (mx - 1)
    inside = jnp.where(lane_c == 0, rotated(xzr[...], turn), rotated(czr[k, 0], 2))
    corner = jnp.where(lane_c == 0, rotated(xyzr[...], turn), rotated(yzr[...], 2))
    ze[mid_c, :] = inside
    ze[0:PAD, :] = corner[my - PAD:my, :]
    below = jnp.zeros((PAD, LANES), jnp.float32)
    last[0, 0:PAD, :] = jnp.broadcast_to(xyr[mx - 1:mx, :], (PAD, LANES))
    last[0, PAD + my:, :] = below

    def rows_last(i, _):
        last[i + 1, 0:PAD, :] = jnp.broadcast_to(cyr[k, 0, pl.ds(i, 1), :], (PAD, LANES))
        last[i + 1, PAD + my:, :] = below
        return 0

    lax.fori_loop(0, mx, rows_last, 0, unroll=8)
    rows_e = my + 2 * PAD
    lane_e = lanes(my + PAD)
    three = 3 if (mx + 1) % 3 == 0 else 1

    def prolong_z(j, _):
        block = last[pl.ds(j * three, three)].reshape(three * rows_e, LANES)
        value = split_dot(block, up)
        for g in range(three):
            outside = 0.5 * rotated(ze[...], lax.rem(LANES - 2 * (j * three + g), LANES))
            for t in range(nt):
                part = value[g * rows_e:g * rows_e + my + PAD, t * LANES:(t + 1) * LANES]
                if t == 0:
                    part = part + jnp.where(lane_e == 0, outside, 0.0)
                q_ref[j * three + g, t] = part
        return 0

    lax.fori_loop(0, (mx + 1) // three, prolong_z, 0)

    for copy, d, _ in sent:
        @pl.when(there(d))
        def _():
            copy(d).wait_send()


def add_kernel(per, smooth_ref, q_ref, out_hbm, both, out_ref, sems):
    mx, nt, my = q_ref.shape[0] - 1, q_ref.shape[1], q_ref.shape[2] - PAD
    ny = 2 * my

    def spread(p, _):
        for t in range(nt):
            here = q_ref[p, t, PAD:PAD + my, :]
            before = q_ref[p, t, PAD - 1:PAD - 1 + my, :]
            both[p, t, pl.ds(0, my, stride=2), :] = 0.5 * (before + here)
            both[p, t, pl.ds(1, my, stride=2), :] = here
        return 0

    def add(j, _):
        for t in range(nt):
            part = pl.ds(t * LANES, LANES)
            here = both[j + 1, t]
            first = smooth_ref[t, 2 * j + 1, PAD:PAD + ny, :]
            second = smooth_ref[t, 2 * j + 2, PAD:PAD + ny, :]
            out_ref[2 * j, :, part] = first + 0.5 * (both[j, t] + here)
            out_ref[2 * j + 1, :, part] = second + here
        return 0

    copies = []
    spread(0, 0)
    for c in range(mx // per):
        lax.fori_loop(c * per + 1, (c + 1) * per + 1, spread, 0, unroll=2)
        lax.fori_loop(c * per, (c + 1) * per, add, 0)
        rows = pl.ds(2 * c * per, 2 * per)
        copies.append(pltpu.make_async_copy(out_ref.at[rows], out_hbm.at[rows], sems.at[c]))
        copies[-1].start()
    for copy in copies:
        copy.wait()


def on_device(sizes, start_field, right_side):
    nx, ny, nz = start_field.shape
    nt, mx, my = nz // LANES, nx // 2, ny // 2
    f32 = jnp.float32
    fine_shape = (nt, nx + 2, ny + 2 * PAD, LANES)
    fine = pltpu.VMEM(fine_shape, f32)
    coarse = pltpu.VMEM((mx + 2, my + 2 * PAD, LANES), f32)
    rounds = FINE_SWEEPS + 1
    y_faces = pltpu.VMEM((rounds, 2, nt, nx, LANES), f32)
    z_pairs = pltpu.VMEM((rounds, 2, ny, LANES), f32)
    x_plane = pltpu.VMEM((nt, ny, LANES), f32)
    y_rows = pltpu.VMEM((nt, mx, LANES), f32)
    z_pack = pltpu.VMEM((my, LANES), f32)
    vmem = pl.BlockSpec(memory_space=pltpu.VMEM)
    smooth, q = pl.pallas_call(
        functools.partial(correct_kernel, sizes),
        out_shape=(
            pltpu.VMEM(fine_shape, f32),
            pltpu.VMEM((mx + 1, nt, my + PAD, LANES), f32),
        ),
        in_specs=[pl.BlockSpec(memory_space=pltpu.HBM)] * 2,
        out_specs=(vmem, vmem),
        scratch_shapes=[
            fine, fine, pltpu.VMEM((nt, nx, ny, LANES), f32),
            y_faces, y_faces, z_pairs, pltpu.VMEM((rounds, 2, 2, ny, LANES), f32), z_pairs,
            x_plane, x_plane, pltpu.VMEM((nt, mx, ny, LANES), f32), pltpu.VMEM((mx, my, nz), f32),
            y_rows, y_rows, y_rows, z_pack, z_pack, pltpu.VMEM((mx, my, LANES), f32),
            coarse, coarse, coarse, coarse,
            pltpu.VMEM((COARSE_SWEEPS, 2, mx, LANES), f32), pltpu.VMEM((COARSE_SWEEPS, 2, mx, LANES), f32),
            pltpu.VMEM((COARSE_SWEEPS, my, LANES), f32), pltpu.VMEM((COARSE_SWEEPS, 2, my, LANES), f32),
            pltpu.VMEM((COARSE_SWEEPS, my, LANES), f32),
            pltpu.VMEM((mx, LANES), f32), z_pack, z_pack, z_pack, pltpu.VMEM((my + PAD, LANES), f32),
            pltpu.SemaphoreType.DMA((4 * nt,)),
            pltpu.SemaphoreType.DMA((N_COPIES,)),
            pltpu.SemaphoreType.DMA((N_COPIES,)),
        ],
        compiler_params=pltpu.CompilerParams(
            collective_id=0, has_side_effects=True, vmem_limit_bytes=40 * 1024 * 1024),
    )(*(pltpu.with_memory_space_constraint(a, pltpu.HBM) for a in (start_field, right_side)))
    per = 8 if mx % 8 == 0 else 1
    return pl.pallas_call(
        functools.partial(add_kernel, per),
        out_shape=jax.ShapeDtypeStruct((nx, ny, nz), f32),
        in_specs=[vmem, vmem],
        out_specs=pl.BlockSpec(memory_space=pl.ANY),
        scratch_shapes=[
            pltpu.VMEM((mx + 1, nt, ny, LANES), f32), pltpu.VMEM((nx, ny, nz), f32),
            pltpu.SemaphoreType.DMA((mx // per,)),
        ],
        compiler_params=pltpu.CompilerParams(vmem_limit_bytes=24 * 1024 * 1024),
    )(smooth, q)


def solution(mesh):
    placed = (P(*AXES), P(*AXES))
    sizes = tuple(mesh.shape[a] for a in AXES)
    return jax.shard_map(
        functools.partial(on_device, sizes), mesh=mesh, in_specs=placed, out_specs=P(*AXES), check_vma=False
    )
```

```python
import functools

import jax
import jax.numpy as jnp
from jax import lax
from jax.experimental import pallas as pl
from jax.experimental.pallas import tpu as pltpu
from jax.sharding import PartitionSpec as P

FINE_SWEEPS = 2
COARSE_SWEEPS = 4
OMEGA = 6.0 / 7.0
STEP = OMEGA / 1.5
LANES = 128
PAD = 8
ROWS = 16
AXES = ("gx", "gy", "gz")
MESH = pl.DeviceIdType.MESH

FACES = ((1, 0, 0), (-1, 0, 0), (0, 1, 0), (0, -1, 0), (0, 0, 1), (0, 0, -1))
EDGES = ((0, 1, 1), (1, 1, 0), (1, 0, 1), (1, 1, 1))
NEIGHBOURS = FACES + EDGES + tuple(tuple(-c for c in d) for d in EDGES)
N_COPIES = 10 * (FINE_SWEEPS + 1) + 4 + 6 * (COARSE_SWEEPS - 1) + 7


def rotated(values, shift):
    return pltpu.roll(values, shift, 1)


def split_dot(values, matrix):
    high = values.astype(jnp.bfloat16)
    rest = values - high.astype(jnp.float32)
    middle = rest.astype(jnp.bfloat16)
    low = (rest - middle.astype(jnp.float32)).astype(jnp.bfloat16)
    total = jnp.dot(low, matrix, preferred_element_type=jnp.float32)
    total = total + jnp.dot(middle, matrix, preferred_element_type=jnp.float32)
    return total + jnp.dot(high, matrix, preferred_element_type=jnp.float32)


def correct_kernel(
    sizes, start_hbm, right_hbm, u2, q_ref,
    u0, u1, f, ys, yr, zs, zr, zm, rk, rs, rr, px, py, rys, ryr, rdr, rzs, rzr, rhs,
    c0, c1, c2, c3, cys, cyr, czs, czr, czm, xyr, xzr, yzr, xyzr, ze,
    local_sem, send_sem, recv_sem,
):
    nt, nx, ny, _ = f.shape
    mx, my = nx // 2, ny // 2
    half = nx // 2
    me = tuple(lax.axis_index(a) for a in AXES)

    def lanes(rows):
        return lax.broadcasted_iota(jnp.int32, (rows, LANES), 1)

    lane, lane_c = lanes(ny), lanes(my)

    def there(d):
        found = None
        for at, step, size in zip(me, d, sizes):
            if step:
                one = at < size - 1 if step > 0 else at > 0
                found = one if found is None else jnp.logical_and(found, one)
        return found

    def minus(d):
        return tuple(-c for c in d)

    def device(d):
        return tuple(at + step for at, step in zip(me, d))

    sent = []

    def send(src, dst, d):
        number = len(sent)

        def copy(to):
            return pltpu.make_async_remote_copy(
                src_ref=src, dst_ref=dst, send_sem=send_sem.at[number],
                recv_sem=recv_sem.at[number], device_id=device(to), device_id_type=MESH)

        @pl.when(there(d))
        def _():
            copy(d).start()

        sent.append((copy, d, dst))
        return number

    def arrive(number):
        copy, d, dst = sent[number]

        @pl.when(there(minus(d)))
        def _():
            copy(minus(d)).wait_recv()

        @pl.when(jnp.logical_not(there(minus(d))))
        def _():
            dst[...] = jnp.zeros(dst.shape, dst.dtype)

    loads = []
    for into, source in ((u0, start_hbm), (f, right_hbm)):
        for h in range(2):
            for t in range(nt):
                rows = pl.ds(h * half, half)
                to = f.at[t, rows] if into is f else u0.at[t, pl.ds(1 + h * half, half), pl.ds(PAD, ny), :]
                loads.append(pltpu.make_async_copy(
                    source.at[rows, :, pl.ds(t * LANES, LANES)], to, local_sem.at[len(loads)]))
    for load in loads:
        load.start()

    barrier = pltpu.get_barrier_semaphore()
    expected = jnp.int32(0)
    for d in NEIGHBOURS:
        @pl.when(there(d))
        def _():
            pl.semaphore_signal(barrier, inc=1, device_id=device(d), device_id_type=MESH)
        expected = expected + there(d).astype(jnp.int32)
    zs[...] = jnp.zeros(zs.shape, zs.dtype)
    czs[...] = jnp.zeros(czs.shape, czs.dtype)
    pl.semaphore_wait(barrier, expected)

    mid = pl.ds(PAD, ny)

    def pack_lanes(ref, at, place, first, last):
        index = lanes(first.shape[0])
        both = rotated(jnp.where(index == LANES - 1, last, first), 2 * place + 1)
        chosen = jnp.logical_or(index == 2 * place, index == 2 * place + 1)
        ref[at] = jnp.where(chosen, both, ref[at])

    def merge_lanes(low, high):
        index = lanes(low.shape[0])
        return jnp.where(lax.rem(index, 2) == 0, low, rotated(high, LANES - 2))

    block = ROWS if ny % ROWS == 0 else ny
    blocks = range(0, ny, block)

    def pack_fine(k, h, x, row, planes):
        for t in range(nt):
            if row == 0:
                ys[k, 0, t, pl.ds(x, 1), :] = planes[t][0:1, :]
            if row == ny - block:
                ys[k, 1, t, pl.ds(x, 1), :] = planes[t][block - 1:block, :]
        pack_lanes(zs, (k, h, pl.ds(row, block)), x - h * half, planes[0], planes[nt - 1])

    def send_low(u):
        return send(u.at[:, 1, mid, :], u.at[:, nx + 1, mid, :], (-1, 0, 0))

    def send_high(u):
        return send(u.at[:, nx, mid, :], u.at[:, 0, mid, :], (1, 0, 0))

    def send_yz(k, h):
        rows = pl.ds(h * half, half)
        return [
            send(ys.at[k, 1, :, rows, :], yr.at[k, 0, :, rows, :], (0, 1, 0)),
            send(ys.at[k, 0, :, rows, :], yr.at[k, 1, :, rows, :], (0, -1, 0)),
            send(zs.at[k, h], zr.at[k, h, 0], (0, 0, 1)),
            send(zs.at[k, h], zr.at[k, h, 1], (0, 0, -1)),
        ]

    def fill_fine(u, k, h, waits):
        for number in waits:
            arrive(number)
        zm[k, h] = merge_lanes(zr[k, h, 0], zr[k, h, 1])

        def rows(x, _):
            for t in range(nt):
                u[t, x + 1, PAD - 1:PAD, :] = yr[k, 0, t, pl.ds(x, 1), :]
                u[t, x + 1, PAD + ny:PAD + ny + 1, :] = yr[k, 1, t, pl.ds(x, 1), :]
            return 0
        lax.fori_loop(h * half, (h + 1) * half, rows, 0, unroll=4)

    lane_b = lanes(block)

    def around(u, k, h, x, row):
        sums = []
        outer = rotated(zm[k, h, pl.ds(row, block), :], lax.rem(LANES - 2 * (x - h * half), LANES))
        here = pl.ds(PAD + row, block)
        planes = [u[t, x + 1, here, :] for t in range(nt)]
        left = [rotated(p, 1) for p in planes]
        right = [rotated(p, LANES - 1) for p in planes]
        for t in range(nt):
            before = jnp.where(lane_b == 0, left[t - 1] if t else outer, left[t])
            after = jnp.where(lane_b == LANES - 1, right[t + 1] if t < nt - 1 else outer, right[t])
            total = u[t, x, here, :] + u[t, x + 2, here, :]
            total = total + u[t, x + 1, pl.ds(PAD - 1 + row, block), :]
            total = total + u[t, x + 1, pl.ds(PAD + 1 + row, block), :]
            sums.append(total + before + after)
        return planes, sums

    waits_yz, low_arrival, high_arrival = [None, None], None, None
    for h in range(2):
        for load in loads[h * nt:(h + 1) * nt]:
            load.wait()

        def pack_start(j, _, h=h):
            for x in (2 * j, 2 * j + 1):
                for row in blocks:
                    pack_fine(0, h, x, row, [u0[t, x + 1, pl.ds(PAD + row, block), :] for t in range(nt)])
            return 0

        lax.fori_loop(h * half // 2, (h + 1) * half // 2, pack_start, 0)
        waits_yz[h] = send_yz(0, h)
        if h == 0:
            high_arrival = send_low(u0)
        else:
            low_arrival = send_high(u0)
    for load in loads[2 * nt:]:
        load.wait()

    fields = (u0, u1, u2)
    for k in range(FINE_SWEEPS):
        old, new = fields[k], fields[k + 1]

        def pair(j, h, old=old, new=new, k=k):
            for row in blocks:
                for x in (2 * j, 2 * j + 1):
                    planes, sums = around(old, k, h, x, row)
                    results = []
                    for t in range(nt):
                        value = (planes[t] + f[t, x, pl.ds(row, block), :] + sums[t]) * (1.0 - OMEGA)
                        new[t, x + 1, pl.ds(PAD + row, block), :] = value
                        results.append(value)
                    pack_fine(k + 1, h, x, row, results)

        next_yz = [None, None]
        fill_fine(old, k, 0, waits_yz[0])
        lax.fori_loop(1, half // 2, lambda j, _: (pair(j, 0), 0)[1], 0)
        arrive(low_arrival)
        pair(0, 0)
        next_yz[0] = send_yz(k + 1, 0)
        next_high = send_low(new)
        arrive(high_arrival)
        fill_fine(old, k, 1, waits_yz[1])
        lax.fori_loop(half // 2, nx // 2, lambda j, _: (pair(j, 1), 0)[1], 0)
        next_yz[1] = send_yz(k + 1, 1)
        low_arrival, high_arrival = send_high(new), next_high
        waits_yz = next_yz

    smooth = fields[FINE_SWEEPS]
    k_last = FINE_SWEEPS

    def residual(x, h, row):
        planes, sums = around(smooth, k_last, h, x, row)
        return [f[t, x, pl.ds(row, block), :] - 6.0 * planes[t] + sums[t] for t in range(nt)]

    def keep(ref, row, values):
        for t in range(nt):
            ref[t, pl.ds(row, block), :] = values[t]

    def step_x(i, h, ref, out):
        for row in blocks:
            even, odd = residual(2 * i, h, row), residual(2 * i + 1, h, row)
            for t in range(nt):
                following = ref[t, pl.ds(row, block), :]
                value = 0.25 * even[t] + 0.5 * odd[t] + 0.25 * following
                px[t, i, pl.ds(row, block), :] = value
                if row == 0:
                    rys[t, pl.ds(i, 1), :] = value[0:1, :]
            keep(out, row, even)

    def start_x(x, h):
        for row in blocks:
            keep(rk, row, residual(x, h, row))

    middle = half // 2
    fill_fine(smooth, k_last, 0, waits_yz[0])
    start_x(half - 2, 0)
    lax.fori_loop(0, middle - 2, lambda j, _: (step_x(middle - 2 - j, 0, rk, rk), 0)[1], 0, unroll=2)
    arrive(low_arrival)
    step_x(0, 0, rk, rs)
    rx = send(rs, rr, (-1, 0, 0))
    arrive(high_arrival)
    fill_fine(smooth, k_last, 1, waits_yz[1])
    start_x(nx - 2, 1)
    lax.fori_loop(0, mx - 1 - middle, lambda j, _: (step_x(mx - 2 - j, 1, rk, rk), 0)[1], 0, unroll=3)
    step_x(middle - 1, 0, rk, rk)
    arrive(rx)
    step_x(mx - 1, 1, rr, rk)
    ry = send(rys, ryr, (0, -1, 0))
    rd = send(rys, rdr, (0, -1, -1))

    def weights(fine, coarse, scale):
        gap = fine - 2 * coarse
        outer = jnp.logical_or(gap == 0, gap == 2)
        value = jnp.where(gap == 1, 0.5 * scale, jnp.where(outer, 0.25 * scale, 0.0))
        return value.astype(jnp.bfloat16)

    nz = nt * LANES
    down = weights(
        lax.broadcasted_iota(jnp.int32, (nz, LANES), 0), lax.broadcasted_iota(jnp.int32, (nz, LANES), 1), 1.0)
    up = weights(
        lax.broadcasted_iota(jnp.int32, (LANES, nz), 1), lax.broadcasted_iota(jnp.int32, (LANES, nz), 0), 2.0)
    last_row = lax.broadcasted_iota(jnp.int32, (my, LANES), 0) == my - 1

    def step_y(i, pack):
        for t in range(nt):
            evens = px[t, i, pl.ds(0, my, stride=2), :]
            odds = px[t, i, pl.ds(1, my, stride=2), :]
            nexts = jnp.where(last_row, 0.0, pltpu.roll(evens, my - 1, 0))
            part = 0.25 * evens + 0.5 * odds + 0.25 * nexts
            py[i, :, t * LANES:(t + 1) * LANES] = part
            if t == 0:
                pack = jnp.where(lane_c == i, rotated(part, i), pack)
        return pack

    zero_c = jnp.zeros((my, LANES), jnp.float32)
    rzs[...] = lax.fori_loop(0, mx, step_y, zero_c, unroll=4)
    rz = send(rzs, rzr, (0, 0, -1))
    group = 4 if mx % 4 == 0 else 1

    def step_z(i, _):
        at = pl.ds(i * group, group)
        rhs[at] = split_dot(py[at].reshape(group * my, nz), down).reshape(group, my, LANES)
        return 0

    lax.fori_loop(0, mx // group, step_z, 0)

    mid_c = pl.ds(PAD, my)

    def pack_coarse(k, i, plane):
        cys[k, 0, pl.ds(i, 1), :] = plane[0:1, :]
        cys[k, 1, pl.ds(i, 1), :] = plane[my - 1:my, :]
        pack_lanes(czs, k, i, plane, plane)

    def send_coarse(c, k):
        return [
            send(c.at[mx, mid_c, :], c.at[0, mid_c, :], (1, 0, 0)),
            send(c.at[1, mid_c, :], c.at[mx + 1, mid_c, :], (-1, 0, 0)),
            send(cys.at[k, 1], cyr.at[k, 0], (0, 1, 0)),
            send(cys.at[k, 0], cyr.at[k, 1], (0, -1, 0)),
            send(czs.at[k], czr.at[k, 0], (0, 0, 1)),
            send(czs.at[k], czr.at[k, 1], (0, 0, -1)),
        ]

    for number in (ry, rd, rz):
        arrive(number)
    beyond = jnp.where(lanes(mx) == LANES - 1, 0.0625 * rotated(rdr[0], LANES - 1), 0.0)
    beyond = beyond + 0.25 * split_dot(jnp.concatenate([ryr[t] for t in range(nt)], 1), down)
    cys[0, 0] = beyond

    def finish_rhs(i, _):
        outside = 0.25 * rotated(rzr[...], LANES - 1 - i)
        value = rhs[i] + jnp.where(lane_c == LANES - 1, outside, 0.0)
        value = value + jnp.where(last_row, cys[0, 0, pl.ds(i, 1), :], 0.0)
        value = value * STEP
        rhs[i] = value
        c0[i + 1, mid_c, :] = value
        pack_coarse(0, i, value)
        return 0

    lax.fori_loop(0, mx, finish_rhs, 0, unroll=4)
    grids = (c0, c1, c2, c3)
    waits = send_coarse(c0, 0)
    for k in range(COARSE_SWEEPS - 1):
        old, new = grids[k], grids[k + 1]
        for number in waits:
            arrive(number)
        czm[k] = merge_lanes(czr[k, 0], czr[k, 1])

        def rows(i, _):
            old[i + 1, PAD - 1:PAD, :] = cyr[k, 0, pl.ds(i, 1), :]
            old[i + 1, PAD + my:PAD + my + 1, :] = cyr[k, 1, pl.ds(i, 1), :]
            return 0

        lax.fori_loop(0, mx, rows, 0, unroll=8)

        def sweep_c(i, _):
            outer = rotated(czm[k], lax.rem(LANES - 2 * i, LANES))
            plane = old[i + 1, mid_c, :]
            total = old[i, mid_c, :] + old[i + 2, mid_c, :]
            total = total + old[i + 1, PAD - 1:PAD - 1 + my, :] + old[i + 1, PAD + 1:PAD + 1 + my, :]
            total = total + jnp.where(lane_c == 0, outer, rotated(plane, 1))
            total = total + jnp.where(lane_c == LANES - 1, outer, rotated(plane, LANES - 1))
            value = (1.0 - 1.5 * STEP) * plane + rhs[i] + (0.25 * STEP) * total
            new[i + 1, mid_c, :] = value
            pack_coarse(k + 1, i, value)
            return 0

        lax.fori_loop(0, mx, sweep_c, 0, unroll=8)
        if k < COARSE_SWEEPS - 2:
            waits = send_coarse(new, k + 1)

    k = COARSE_SWEEPS - 1
    last = grids[k]
    waits = [
        send(last.at[mx, mid_c, :], last.at[0, mid_c, :], (1, 0, 0)),
        send(cys.at[k, 1], cyr.at[k, 0], (0, 1, 0)),
        send(czs.at[k], czr.at[k, 0], (0, 0, 1)),
        send(cys.at[k, 1], xyr, (1, 1, 0)),
        send(czs.at[k], xzr, (1, 0, 1)),
        send(czs.at[k], yzr, (0, 1, 1)),
        send(czs.at[k], xyzr, (1, 1, 1)),
    ]
    for number in waits:
        arrive(number)
    turn = LANES - 2 * (mx - 1)
    inside = jnp.where(lane_c == 0, rotated(xzr[...], turn), rotated(czr[k, 0], 2))
    corner = jnp.where(lane_c == 0, rotated(xyzr[...], turn), rotated(yzr[...], 2))
    ze[mid_c, :] = inside
    ze[0:PAD, :] = corner[my - PAD:my, :]
    below = jnp.zeros((PAD, LANES), jnp.float32)
    last[0, 0:PAD, :] = jnp.broadcast_to(xyr[mx - 1:mx, :], (PAD, LANES))
    last[0, PAD + my:, :] = below

    def rows_last(i, _):
        last[i + 1, 0:PAD, :] = jnp.broadcast_to(cyr[k, 0, pl.ds(i, 1), :], (PAD, LANES))
        last[i + 1, PAD + my:, :] = below
        return 0

    lax.fori_loop(0, mx, rows_last, 0, unroll=8)
    rows_e = my + 2 * PAD
    lane_e = lanes(my + PAD)
    three = 3 if (mx + 1) % 3 == 0 else 1

    def prolong_z(j, _):
        value = split_dot(last[pl.ds(j * three, three)].reshape(three * rows_e, LANES), up)
        for g in range(three):
            outside = 0.5 * rotated(ze[...], lax.rem(LANES - 2 * (j * three + g), LANES))
            for t in range(nt):
                part = value[g * rows_e:g * rows_e + my + PAD, t * LANES:(t + 1) * LANES]
                if t == 0:
                    part = part + jnp.where(lane_e == 0, outside, 0.0)
                q_ref[j * three + g, t] = part
        return 0

    lax.fori_loop(0, (mx + 1) // three, prolong_z, 0)

    for copy, d, _ in sent:
        @pl.when(there(d))
        def _():
            copy(d).wait_send()


def add_kernel(per, smooth_ref, q_ref, out_hbm, both, out_ref, sems):
    mx, nt, my = q_ref.shape[0] - 1, q_ref.shape[1], q_ref.shape[2] - PAD
    ny = 2 * my

    def spread(p, _):
        for t in range(nt):
            here = q_ref[p, t, PAD:PAD + my, :]
            before = q_ref[p, t, PAD - 1:PAD - 1 + my, :]
            both[p, t, pl.ds(0, my, stride=2), :] = 0.5 * (before + here)
            both[p, t, pl.ds(1, my, stride=2), :] = here
        return 0

    def add(j, _):
        for t in range(nt):
            part = pl.ds(t * LANES, LANES)
            here = both[j + 1, t]
            first = smooth_ref[t, 2 * j + 1, PAD:PAD + ny, :]
            second = smooth_ref[t, 2 * j + 2, PAD:PAD + ny, :]
            out_ref[2 * j, :, part] = first + 0.5 * (both[j, t] + here)
            out_ref[2 * j + 1, :, part] = second + here
        return 0

    copies = []
    spread(0, 0)
    for c in range(mx // per):
        lax.fori_loop(c * per + 1, (c + 1) * per + 1, spread, 0, unroll=2)
        lax.fori_loop(c * per, (c + 1) * per, add, 0)
        rows = pl.ds(2 * c * per, 2 * per)
        copies.append(pltpu.make_async_copy(out_ref.at[rows], out_hbm.at[rows], sems.at[c]))
        copies[-1].start()
    for copy in copies:
        copy.wait()


def on_device(sizes, start_field, right_side):
    nx, ny, nz = start_field.shape
    nt, mx, my = nz // LANES, nx // 2, ny // 2
    f32 = jnp.float32
    fine_shape = (nt, nx + 2, ny + 2 * PAD, LANES)
    fine = pltpu.VMEM(fine_shape, f32)
    coarse = pltpu.VMEM((mx + 2, my + 2 * PAD, LANES), f32)
    rounds = FINE_SWEEPS + 1
    y_faces = pltpu.VMEM((rounds, 2, nt, nx, LANES), f32)
    z_pairs = pltpu.VMEM((rounds, 2, ny, LANES), f32)
    x_plane = pltpu.VMEM((nt, ny, LANES), f32)
    y_rows = pltpu.VMEM((nt, mx, LANES), f32)
    z_pack = pltpu.VMEM((my, LANES), f32)
    vmem = pl.BlockSpec(memory_space=pltpu.VMEM)
    smooth, q = pl.pallas_call(
        functools.partial(correct_kernel, sizes),
        out_shape=(
            pltpu.VMEM(fine_shape, f32),
            pltpu.VMEM((mx + 1, nt, my + PAD, LANES), f32),
        ),
        in_specs=[pl.BlockSpec(memory_space=pltpu.HBM)] * 2,
        out_specs=(vmem, vmem),
        scratch_shapes=[
            fine, fine, pltpu.VMEM((nt, nx, ny, LANES), f32),
            y_faces, y_faces, z_pairs, pltpu.VMEM((rounds, 2, 2, ny, LANES), f32), z_pairs,
            x_plane, x_plane, x_plane, pltpu.VMEM((nt, mx, ny, LANES), f32), pltpu.VMEM((mx, my, nz), f32),
            y_rows, y_rows, y_rows, z_pack, z_pack, pltpu.VMEM((mx, my, LANES), f32),
            coarse, coarse, coarse, coarse,
            pltpu.VMEM((COARSE_SWEEPS, 2, mx, LANES), f32), pltpu.VMEM((COARSE_SWEEPS, 2, mx, LANES), f32),
            pltpu.VMEM((COARSE_SWEEPS, my, LANES), f32), pltpu.VMEM((COARSE_SWEEPS, 2, my, LANES), f32),
            pltpu.VMEM((COARSE_SWEEPS, my, LANES), f32),
            pltpu.VMEM((mx, LANES), f32), z_pack, z_pack, z_pack, pltpu.VMEM((my + PAD, LANES), f32),
            pltpu.SemaphoreType.DMA((4 * nt,)),
            pltpu.SemaphoreType.DMA((N_COPIES,)),
            pltpu.SemaphoreType.DMA((N_COPIES,)),
        ],
        compiler_params=pltpu.CompilerParams(
            collective_id=0, has_side_effects=True, vmem_limit_bytes=40 * 1024 * 1024),
    )(*(pltpu.with_memory_space_constraint(a, pltpu.HBM) for a in (start_field, right_side)))
    per = 8 if mx % 8 == 0 else 1
    return pl.pallas_call(
        functools.partial(add_kernel, per),
        out_shape=jax.ShapeDtypeStruct((nx, ny, nz), f32),
        in_specs=[vmem, vmem],
        out_specs=pl.BlockSpec(memory_space=pl.ANY),
        scratch_shapes=[
            pltpu.VMEM((mx + 1, nt, ny, LANES), f32), pltpu.VMEM((nx, ny, nz), f32),
            pltpu.SemaphoreType.DMA((mx // per,)),
        ],
        compiler_params=pltpu.CompilerParams(vmem_limit_bytes=24 * 1024 * 1024),
    )(smooth, q)


def solution(mesh):
    placed = (P(*AXES), P(*AXES))
    sizes = tuple(mesh.shape[a] for a in AXES)
    return jax.shard_map(
        functools.partial(on_device, sizes), mesh=mesh, in_specs=placed, out_specs=P(*AXES), check_vma=False
    )
```
